32 devices in a mesh: pair: 4 (over x, core), row: 8 (over z, y).
Axes of the slice: x: 2, y: 2, z: 4, core: 2. Of those that a mesh axis runs over, the one named last changes fastest.
Arguments:
- descriptors: bfloat16 [32, 2048, 256], P('pair', 'row'), parts along dimension 0, may hold values from -8 to 8
- counts: int32 [32], P('pair'), parts along dimension 0, may hold values from 512 to 2048
- pairs: int32 [16, 2], P('pair'), parts along dimension 0, may hold values from 0 to 7, as said below
- bin_score: float32 [1], replicated, may hold values from 0.5 to 2
Outputs:
- log_match: float32 [16, 2048, 2048], P('pair', 'row'), parts along dimension 0
- row_bins: float32 [16, 2048], P('pair', 'row'), parts along dimension 0
- col_bins: float32 [16, 2048], P('pair'), parts along dimension 0
The draws below stay inside these ranges and needn't reach their ends.
There are 4 independent parts, one for each index of `pair`. The reference program is written for one: setup_inputs(seed, part) draws one part's arguments, and reference() takes and returns one part's arrays. A program takes and returns all parts, laid end to end along the dimension named above; an argument that names none is the same for every part. Nothing has to cross between parts.
Inputs may be any that keep to these rules, and one draw needn't show every extreme that they name: Image k's keypoints are its first counts[k] slots. `pairs`: the two images of a pair differ.
All inputs are finite; a program needn't handle non-finite values.
Results may differ from the reference program's by a relative error of at most 0.0003.
Values may be sent and summed in bfloat16 or wider, within the bound.
A program may use at most 64 MiB of HBM per device.

```python
import jax
import jax.numpy as jnp
from jax import lax

PAIRS = 4
IMAGES = 8
KP = 2048
D = 256
ITERS = 10


def draw_descriptors(key, part):
    values = 2.0 * jax.random.truncated_normal(jax.random.fold_in(key, 5), -4.0, 4.0, (IMAGES, KP, D), jnp.float32)
    return values.astype(jnp.bfloat16)


def draw_pairs(key, part):
    first_image = jax.random.randint(jax.random.fold_in(key, 1), (PAIRS,), 0, IMAGES)
    stride = jax.random.randint(jax.random.fold_in(key, 2), (PAIRS,), 1, IMAGES)
    second_image = (first_image + stride) % IMAGES
    return jnp.stack([first_image, second_image], axis=1).astype(jnp.int32)


def set_ends(entries, key, least, largest):
    spot = [jax.random.randint(jax.random.fold_in(key, axis), (), 0, length) for axis, length in enumerate(entries.shape)]
    longest = entries.shape.index(max(entries.shape))
    neighbour = spot[:longest] + [(spot[longest] + 1) % entries.shape[longest]] + spot[longest + 1:]
    return entries.at[tuple(spot)].set(least).at[tuple(neighbour)].set(largest)


def setup_inputs(seed: int = 0, part: int = 0) -> dict:
    keys = jax.random.split(jax.random.key(seed), 5)
    part_splits = jax.random.split(jax.random.fold_in(keys[4], part), 5)
    descriptors = draw_descriptors(jax.random.fold_in(jax.random.fold_in(keys[4], part), 71), part)
    counts = set_ends(jax.random.randint(part_splits[1], (IMAGES,), KP // 4, KP + 1), jax.random.fold_in(part_splits[1], 1), KP // 4, KP).astype(jnp.int32)
    pairs = draw_pairs(jax.random.fold_in(jax.random.fold_in(keys[4], part), 71), part)
    bin_score = jnp.clip(jax.random.uniform(keys[3], (1,), jnp.float32, 0.5, 2.0), 0.5, 2.0)
    return dict(descriptors=descriptors, counts=counts, pairs=pairs, bin_score=bin_score)


NEG = -1.0e30


def masked_lse(values, kept, reduce_dim):
    held = jnp.where(kept, values, NEG)
    ceiling = jnp.max(held, axis=reduce_dim, keepdims=True)
    summed = jnp.sum(jnp.where(kept, jnp.exp(held - ceiling), 0.0), axis=reduce_dim, keepdims=True)
    return jnp.squeeze(ceiling + jnp.log(summed), reduce_dim)


def reference(descriptors, counts, pairs, bin_score):
    bin_value = bin_score[0]
    row_images = descriptors[pairs[:, 0]]
    col_images = descriptors[pairs[:, 1]]
    row_counts = counts[pairs[:, 0]]
    col_counts = counts[pairs[:, 1]]

    def one_pair(operands):
        row_desc, col_desc, n_rows, n_cols = operands
        scores = jnp.dot(row_desc, col_desc.T, preferred_element_type=jnp.float32) * (D ** -0.5)
        side_line = jnp.zeros((KP, 1), jnp.float32) + bin_value
        upper = jnp.concatenate([scores, side_line], axis=1)
        bin_line = jnp.zeros((1, KP + 1), jnp.float32) + bin_value
        couplings = jnp.concatenate([upper, bin_line], axis=0)
        cell_index = jnp.arange(KP + 1, dtype=jnp.int32)
        row_kept = (cell_index < n_rows) | (cell_index == KP)
        col_kept = (cell_index < n_cols) | (cell_index == KP)
        row_count = n_rows.astype(jnp.float32)
        col_count = n_cols.astype(jnp.float32)
        log_norm = -jnp.log(row_count + col_count)
        log_mu = jnp.where(cell_index == KP, jnp.log(col_count) + log_norm, log_norm)
        log_nu = jnp.where(cell_index == KP, jnp.log(row_count) + log_norm, log_norm)
        row_pot = jnp.zeros((KP + 1,), jnp.float32)
        col_pot = jnp.zeros((KP + 1,), jnp.float32)
        for sweep_index in range(ITERS):
            row_pot = log_mu - masked_lse(couplings + col_pot[None, :], col_kept[None, :], 1)
            col_pot = log_nu - masked_lse(couplings + row_pot[:, None], row_kept[:, None], 0)
        assign = couplings + row_pot[:, None] + col_pot[None, :] - log_norm
        assign = jnp.where(row_kept[:, None] & col_kept[None, :], assign, 0.0)
        return assign[:KP, :KP], assign[:KP, KP], assign[KP, :KP]

    log_match, row_bins, col_bins = lax.map(one_pair, (row_images, col_images, row_counts, col_counts))
    return (log_match, row_bins, col_bins)
```

```python
import functools

import jax
import jax.numpy as jnp
from jax import lax
from jax.experimental import pallas as pl
from jax.experimental.pallas import tpu as pltpu
from jax.sharding import PartitionSpec as P

ITERS = 10
LIFT = 40.0
LANES = 128
BLOCK = 128
MESH = pl.DeviceIdType.MESH
NT = (((1,), (1,)), ((), ()))


def sinkhorn_kernel(
    teams, size, counts, pairs, bin_score, desc, imgs, fin,
    rowsel, colsel, rows, own, kern, peak, kbin, mass, left, b8, bbin, abin, xbuf, fin_send,
    crit_send, crit_recv, fwd_send, fwd_recv, bulk_send, bulk_recv, ex_send, ex_recv, fin_ssem, fin_rsem, local_sem,
):
    me = lax.axis_index("row")
    team, member = me // size, me % size
    local, depth = rows.shape[1], rows.shape[2]
    height, cols = kern.shape
    blocks = height // BLOCK

    def device(t, m):
        return {"row": t * size + m}

    def remote(src, dst, ssem, rsem, t, m):
        return pltpu.make_async_remote_copy(
            src_ref=src, dst_ref=dst, send_sem=ssem, recv_sem=rsem, device_id=device(t, m), device_id_type=MESH
        )

    barrier = pltpu.get_barrier_semaphore()
    for dz in range(1, teams):
        pl.semaphore_signal(barrier, inc=1, device_id=device((team + dz) % teams, member), device_id_type=MESH)
    for d in range(1, size):
        pl.semaphore_signal(barrier, inc=1, device_id=device(team, (member + d) % size), device_id_type=MESH)

    for p in range(teams):
        colsel[p] = desc[pairs[p, 1]]
        rowsel[p] = desc[pairs[p, 0]]
    own[team, member] = colsel[team]
    rows[team] = rowsel[team]
    pl.semaphore_wait(barrier, teams + size - 2)

    crit = {}
    for dz in range(1, teams):
        to = (team + dz) % teams
        crit[0, dz] = remote(colsel.at[to], own.at[team, member], crit_send.at[0, dz], crit_recv.at[0, dz], to, member)
        crit[0, dz].start()
    for dz in range(1, teams):
        to = (team + dz) % teams
        crit[1, dz] = remote(rowsel.at[to], rows.at[team], crit_send.at[1, dz], crit_recv.at[1, dz], to, member)
        crit[1, dz].start()
    fwd = {}
    for dz in range(teams):
        if dz:
            crit[0, dz].wait_recv()
        source = (team + teams - dz) % teams
        for d in range(1, size):
            fwd[dz, d] = remote(
                own.at[source, member], own.at[source, member], fwd_send.at[dz, d], fwd_recv.at[dz, d],
                team, (member + d) % size,
            )
            fwd[dz, d].start()

    hops = (teams - 1) // 2
    split = teams % 2 == 0
    half = (size + 1) // 2

    def bulk(way, hop, d):
        step = 1 if way == 0 else teams - 1
        to = (team + step) % teams
        image = (team + (teams - step) * hop) % teams
        part = (member + d) % size
        src = own.at[:, part] if hop == 0 else imgs.at[image, :, part]
        return remote(src, imgs.at[image, :, part], bulk_send.at[way, hop, d], bulk_recv.at[way, hop, d], to, member)

    def carried(way, hop):
        if hop < hops:
            return list(range(size))
        if hop == hops and split:
            return list(range(half)) if way == 0 else list(range(half, size))
        return []

    for way in (0, 1):
        if 0 in carried(way, 0):
            bulk(way, 0, 0).start()
    for dz in range(teams):
        for d in range(1, size):
            fwd[dz, d].wait_recv()
    for d in range(1, size):
        for way in (0, 1):
            if d in carried(way, 0):
                bulk(way, 0, d).start()
    keep = pltpu.make_async_copy(own, imgs.at[team], local_sem)
    keep.start()
    for dz in range(1, teams):
        crit[1, dz].wait_recv()

    na_i, nb_i = counts[pairs[team, 0]], counts[pairs[team, 1]]
    line = jnp.ones((1, LANES), jnp.float32)
    na, nb = line * na_i.astype(jnp.float32), line * nb_i.astype(jnp.float32)
    norm = 1.0 / (na + nb)
    mu_bin, nu_bin = nb * norm, na * norm
    bin_value = bin_score[0]
    wide = lax.broadcasted_iota(jnp.int32, (8, cols), 1) < nb_i

    chunk = 512 if cols % 512 == 0 else LANES * size
    per = chunk // local
    flat = own.reshape(teams * size * local, depth)

    @pl.loop(0, teams)
    def _(s):
        block = rows[s]

        @pl.loop(0, cols // chunk)
        def _(n):
            at = pl.multiple_of(n * chunk, chunk)
            part = lax.dot_general(block, flat[pl.ds(at, chunk), :], NT, preferred_element_type=jnp.float32)
            kern[pl.ds(pl.multiple_of(s * local, local), local), pl.ds(at, chunk)] = part * (depth ** -0.5)

    def tree(terms, op):
        while len(terms) > 1:
            terms = [op(terms[i], terms[i + 1]) if i + 1 < len(terms) else terms[i] for i in range(0, len(terms), 2)]
        return terms[0]

    def lanes(x):
        return [x[:, i * LANES : (i + 1) * LANES] for i in range(cols // LANES)]

    @pl.loop(0, height // 64)
    def _(g):
        for i in range(8):
            at = pl.multiple_of(g * 64 + i * 8, 8)
            x = jnp.where(wide, kern[pl.ds(at, 8), :], -1e30)
            top = jnp.max(tree(lanes(x), jnp.maximum), axis=1, keepdims=True)
            top = jnp.maximum(top, bin_value) - LIFT
            kern[pl.ds(at, 8), :] = jnp.exp(x - top)
            peak[pl.ds(at, 8), :] = top
            kbin[pl.ds(at, 8), :] = jnp.exp(bin_value - top)
            slot = at // local
            index = (slot * size + member) * local + at % local + lax.broadcasted_iota(jnp.int32, (8, 1), 0)
            mass[pl.ds(at, 8), :] = jnp.where(index < na_i, norm[:, :1], 0.0)

    b8[...] = jnp.where(wide, 1.0, 0.0)
    bbin[...] = jnp.ones_like(bbin)

    def row_part(g):
        for i in range(BLOCK // 8):
            at = pl.multiple_of(g * BLOCK + i * 8, 8)
            total = jnp.sum(tree(lanes(kern[pl.ds(at, 8), :] * b8[...]), jnp.add), axis=1, keepdims=True)
            total = total + kbin[pl.ds(at, 8), :] * bbin[:, :1]
            left[pl.ds(at, 8), :] = mass[pl.ds(at, 8), :] / total

    def col_part(g, sums):
        acc, edge = sums
        for i in range(BLOCK // 8):
            at = pl.multiple_of(g * BLOCK + i * 8, 8)
            a = left[pl.ds(at, 8), :]
            acc = acc + kern[pl.ds(at, 8), :] * a
            edge = edge + kbin[pl.ds(at, 8), :] * a
        return acc, edge

    def exchange(slot, d):
        return remote(
            xbuf.at[slot, member], xbuf.at[slot, member], ex_send.at[slot, d], ex_recv.at[slot, d],
            team, (member + d) % size,
        )

    def sweep(it, _):
        slot = it % 2
        row_part(0)

        def step(g, sums):
            sums = col_part(g - 1, sums)
            row_part(g)
            return sums

        sums = (jnp.zeros((8, cols), jnp.float32), jnp.zeros((8, 1), jnp.float32))
        sums = lax.fori_loop(1, blocks, step, sums)
        acc, edge = col_part(blocks - 1, sums)
        xbuf[slot, member, :, :cols] = jnp.sum(acc, axis=0, keepdims=True)
        xbuf[slot, member, :, cols:] = jnp.broadcast_to(jnp.sum(edge, axis=0, keepdims=True), (1, LANES))
        for d in range(1, size):
            exchange(slot, d).start()
        all_b = jnp.sum(tree(lanes(b8[0:1, :]), jnp.add), axis=1, keepdims=True) + bbin[0:1, :1]
        row_bin = mu_bin / all_b
        abin[...] = row_bin
        for hop in range(1, teams):
            for way in (0, 1):
                for d in carried(way, hop):
                    @pl.when(it == min(ITERS - 1, 4 * hop + d))
                    def _():
                        bulk(way, hop - 1, d).wait_recv()
                        bulk(way, hop, d).start()
        for d in range(1, size):
            exchange(slot, d).wait()
        total = xbuf[slot, 0]
        for k in range(1, size):
            total = total + xbuf[slot, k]
        total = total + row_bin[:, :1]
        fresh = norm[:, :1] / total[:, :cols]
        fin_send[0, :, :cols] = fresh
        b8[...] = jnp.where(wide, fresh, 0.0)
        bbin[...] = jnp.broadcast_to(nu_bin / total[:, cols:], bbin.shape)
        return 0

    lax.fori_loop(0, ITERS, sweep, 0)

    col_pot = jnp.log(fin_send[0, :, :cols])
    col_bin = jnp.log(bbin[0:1, :])
    row_bin = jnp.log(abin[...]) - bin_value
    eye = lax.broadcasted_iota(jnp.int32, (LANES, LANES), 0) == lax.broadcasted_iota(jnp.int32, (LANES, LANES), 1)
    for t in range(teams):
        fin_send[t, :, :cols] = col_pot
        fin_send[t, :, cols : cols + LANES] = col_bin
        fin_send[t, :, cols + LANES : cols + 2 * LANES] = row_bin
        for i in range(local // LANES):
            at = pl.ds(t * local + i * LANES, LANES)
            pot = jnp.log(jnp.maximum(left[at, :], 1e-37)) - peak[at, :]
            flat_pot = jnp.sum(jnp.where(eye, pot, 0.0), axis=0, keepdims=True)
            fin_send[t, :, cols + (2 + i) * LANES : cols + (3 + i) * LANES] = flat_pot
    sent = []
    for dz in range(1, teams):
        to = (team + dz) % teams
        sent.append(remote(fin_send.at[to], fin.at[team], fin_ssem.at[dz], fin_rsem.at[dz], to, member))
        sent[-1].start()
    fin[team] = fin_send[team]

    for dz in range(1, teams):
        crit[0, dz].wait_send()
        crit[1, dz].wait_send()
    for dz in range(teams):
        for d in range(1, size):
            fwd[dz, d].wait_send()
    keep.wait()
    for hop in range(teams):
        for way in (0, 1):
            for d in carried(way, hop):
                bulk(way, hop, d).wait_send()
                if d not in carried(way, hop + 1):
                    bulk(way, hop, d).wait_recv()
    for copy in sent:
        copy.wait()


def finish_kernel(size, counts, pairs, bin_score, rowdesc, image, fin, log_match, row_bins, col_bins):
    p = pl.program_id(0)
    me = lax.axis_index("row")
    local, depth = rowdesc.shape[1:]
    cols = log_match.shape[2]
    na_i, nb_i = counts[pairs[p, 0]], counts[pairs[p, 1]]
    line = jnp.ones((1, LANES), jnp.float32)
    log_norm = -jnp.log(line * (na_i + nb_i).astype(jnp.float32))[:, :1]
    bin_value = bin_score[0]
    col_pot = fin[0, :, :cols]
    col_bin = fin[0, :, cols : cols + 1]
    row_bin = fin[0, :, cols + LANES : cols + LANES + 1]
    flat_pot = fin[0, :, cols + 2 * LANES :]
    wide = lax.broadcasted_iota(jnp.int32, (1, cols), 1) < nb_i
    row_index = me * local + lax.broadcasted_iota(jnp.int32, (1, local), 1)
    row_bins[pl.ds(p, 1), :] = jnp.where(row_index < na_i, bin_value + flat_pot + col_bin - log_norm, 0.0)
    col_bins[pl.ds(p, 1), :] = jnp.where(wide, bin_value + row_bin + col_pot - log_norm, 0.0)
    eye = lax.broadcasted_iota(jnp.int32, (LANES, LANES), 0) == lax.broadcasted_iota(jnp.int32, (LANES, LANES), 1)
    tops = []
    for i in range(local // LANES):
        piece = flat_pot[:, i * LANES : (i + 1) * LANES]
        tops.append(jnp.sum(jnp.where(eye, piece, 0.0), axis=1, keepdims=True))
    row_pot = jnp.concatenate(tops, axis=0)
    tall = me * local + lax.broadcasted_iota(jnp.int32, (local, 1), 0) < na_i
    flat = image.reshape(cols, depth)
    chunk = 512 if cols % 512 == 0 else LANES
    block = rowdesc[0]
    for n in range(cols // chunk):
        at = slice(n * chunk, (n + 1) * chunk)
        scores = lax.dot_general(block, flat[at, :], NT, preferred_element_type=jnp.float32) * (depth ** -0.5)
        value = scores + row_pot + col_pot[:, at] - log_norm
        log_match[0, :, at] = jnp.where(tall & wide[:, at], value, 0.0)


def on_device(teams, size, descriptors, counts, pairs, bin_score):
    images, local, depth = descriptors.shape
    cols = local * teams * size
    height = local * teams
    width = cols + 2 * LANES + local
    vmem = pl.BlockSpec(memory_space=pltpu.VMEM)
    smem = pl.BlockSpec(memory_space=pltpu.SMEM)
    f32, bf16 = jnp.float32, jnp.bfloat16
    dma = pltpu.SemaphoreType.DMA
    imgs, fin = pl.pallas_call(
        functools.partial(sinkhorn_kernel, teams, size),
        out_shape=(
            jax.ShapeDtypeStruct((teams, teams, size, local, depth), bf16),
            jax.ShapeDtypeStruct((teams, 1, width), f32),
        ),
        in_specs=[smem, smem, smem, vmem],
        out_specs=(pl.BlockSpec(memory_space=pl.ANY), vmem),
        scratch_shapes=[
            pltpu.VMEM((teams, local, depth), bf16),
            pltpu.VMEM((teams, local, depth), bf16),
            pltpu.VMEM((teams, local, depth), bf16),
            pltpu.VMEM((teams, size, local, depth), bf16),
            pltpu.VMEM((height, cols), f32),
            pltpu.VMEM((height, 1), f32),
            pltpu.VMEM((height, 1), f32),
            pltpu.VMEM((height, 1), f32),
            pltpu.VMEM((height, 1), f32),
            pltpu.VMEM((8, cols), f32),
            pltpu.VMEM((8, LANES), f32),
            pltpu.VMEM((1, LANES), f32),
            pltpu.VMEM((2, size, 1, cols + LANES), f32),
            pltpu.VMEM((teams, 1, width), f32),
            dma((2, teams)),
            dma((2, teams)),
            dma((teams, size)),
            dma((teams, size)),
            dma((2, teams, size)),
            dma((2, teams, size)),
            dma((2, size)),
            dma((2, size)),
            dma((teams,)),
            dma((teams,)),
            dma,
        ],
        compiler_params=pltpu.CompilerParams(
            collective_id=0, has_side_effects=True, vmem_limit_bytes=48 * 1024 * 1024
        ),
    )(counts, pairs, bin_score, descriptors)
    return pl.pallas_call(
        functools.partial(finish_kernel, size),
        out_shape=(
            jax.ShapeDtypeStruct((teams, local, cols), f32),
            jax.ShapeDtypeStruct((teams, local), f32),
            jax.ShapeDtypeStruct((teams, cols), f32),
        ),
        grid_spec=pltpu.PrefetchScalarGridSpec(
            num_scalar_prefetch=3,
            grid=(teams,),
            in_specs=[
                pl.BlockSpec((1, local, depth), lambda p, c, q, b: (q[p, 0], 0, 0)),
                pl.BlockSpec((1, teams, size, local, depth), lambda p, c, q, b: (p, 0, 0, 0, 0)),
                pl.BlockSpec((1, 1, width), lambda p, c, q, b: (p, 0, 0)),
            ],
            out_specs=(
                pl.BlockSpec((1, local, cols), lambda p, c, q, b: (p, 0, 0)),
                pl.BlockSpec((teams, local), lambda p, c, q, b: (0, 0)),
                pl.BlockSpec((teams, cols), lambda p, c, q, b: (0, 0)),
            ),
        ),
    )(counts, pairs, bin_score, descriptors, imgs, fin)


def solution(mesh):
    group = mesh.shape["row"]

    def body(descriptors, counts, pairs, bin_score):
        teams = pairs.shape[0]
        return on_device(teams, group // teams, descriptors, counts, pairs, bin_score)

    return jax.shard_map(
        body,
        mesh=mesh,
        in_specs=(P("pair", "row", None), P("pair"), P("pair", None), P()),
        out_specs=(P("pair", "row", None), P("pair", "row"), P("pair", None)),
        check_vma=False,
    )
```

```python
import functools

import jax
import jax.numpy as jnp
from jax import lax
from jax.experimental import pallas as pl
from jax.experimental.pallas import tpu as pltpu
from jax.sharding import PartitionSpec as P

ITERS = 10
LIFT = 40.0
LANES = 128
BLOCK = 128
MESH = pl.DeviceIdType.MESH
NT = (((1,), (1,)), ((), ()))


def sinkhorn_kernel(
    teams, size, counts, pairs, bin_score, desc, imgs, fin,
    rowsel, colsel, rows, own, score, kern, peak, kbin, mass, left, part, b8, bbin, abin, fin_send,
    crit_send, crit_recv, fwd_send, fwd_recv, bulk_send, bulk_recv, side_send, side_recv, fin_ssem, fin_rsem, local_sem,
):
    me = lax.axis_index("row")
    team, member = me // size, me % size
    local, depth = rows.shape[2:]
    height, cols = kern.shape
    blocks = height // BLOCK

    def device(t, m):
        return {"row": t * size + m}

    def remote(src, dst, ssem, rsem, t, m):
        return pltpu.make_async_remote_copy(
            src_ref=src, dst_ref=dst, send_sem=ssem, recv_sem=rsem, device_id=device(t, m), device_id_type=MESH
        )

    barrier = pltpu.get_barrier_semaphore()
    for dz in range(1, teams):
        pl.semaphore_signal(barrier, inc=1, device_id=device((team + dz) % teams, member), device_id_type=MESH)
    for d in range(1, size):
        pl.semaphore_signal(barrier, inc=1, device_id=device(team, (member + d) % size), device_id_type=MESH)

    for p in range(teams):
        colsel[p] = desc[pairs[p, 1]]
        rowsel[p] = desc[pairs[p, 0]]
    own[team, member] = colsel[team]
    rows[team, member] = rowsel[team]
    pl.semaphore_wait(barrier, teams + size - 2)

    def near(k, sign):
        pick = 0
        for t in range(teams):
            ranked = sorted((o for o in range(teams) if o != t), key=lambda o: (abs(o - t), o))
            pick = pick + jnp.where(team == t, sign * (ranked[k] - t) % teams, 0)
        return pick

    held = ((colsel, own), (rowsel, rows))
    ranks = range(teams - 1)

    def crit(kind, dz):
        to = (team + dz) % teams
        src, dst = held[kind]
        return remote(src.at[to], dst.at[team, member], crit_send.at[kind, dz], crit_recv.at[kind, dz], to, member)

    def fwd(kind, dz, d):
        slot = held[kind][1].at[(team + teams - dz) % teams, member]
        return remote(slot, slot, fwd_send.at[kind, dz, d], fwd_recv.at[kind, dz, d], team, (member + d) % size)

    def hand_over(kind, dz):
        for d in range(1, size):
            fwd(kind, dz, d).start()

    for kind in (0, 1):
        for k in reversed(ranks):
            crit(kind, near(k, 1)).start()
        hand_over(kind, 0)

    def bulk(dz, e):
        to = (team + dz) % teams
        image = (to + e) % teams
        return remote(colsel.at[image], imgs.at[image, team, member], bulk_send.at[dz, e], bulk_recv.at[dz, e], to, member)

    def side(dz, e, d):
        source, image = (team + teams - dz) % teams, (team + e) % teams
        slot = imgs.at[image, source, member]
        src = slot if dz else colsel.at[image]
        return remote(src, slot, side_send.at[dz, e, d], side_recv.at[dz, e, d], team, (member + d) % size)

    def pass_on(dz, e):
        for d in range(1, size):
            side(dz, e, d).start()

    order = [(dz, e) for e in range(1, teams) for dz in range(1, teams)]
    for dz, e in order:
        bulk(dz, e).start()
    keeps = []
    for e in range(1, teams):
        image = (team + e) % teams
        keeps.append(pltpu.make_async_copy(colsel.at[image], imgs.at[image, team, member], local_sem.at[e]))
        keeps[-1].start()
    for k in ranks:
        dz = near(k, -1)
        crit(0, dz).wait_recv()
        hand_over(0, dz)

    na_i, nb_i = counts[pairs[team, 0]], counts[pairs[team, 1]]
    line = jnp.ones((1, LANES), jnp.float32)
    na, nb = line * na_i.astype(jnp.float32), line * nb_i.astype(jnp.float32)
    norm = 1.0 / (na + nb)
    mu_bin, nu_bin = nb * norm, na * norm
    bin_value = bin_score[0]
    wide = lax.broadcasted_iota(jnp.int32, (8, cols), 1) < nb_i
    chunk = 512 if cols % 512 == 0 else LANES
    flat = own.reshape(cols, depth)
    spans = range(cols // LANES)

    def tree(terms, op):
        while len(terms) > 1:
            terms = [op(terms[i], terms[i + 1]) if i + 1 < len(terms) else terms[i] for i in range(0, len(terms), 2)]
        return terms[0]

    def lanes(x):
        return [x[:, i * LANES : (i + 1) * LANES] for i in spans]

    def prepare(source, m):
        s = source * size + m
        block = rows[source, m]

        @pl.loop(0, cols // chunk)
        def _(n):
            at = pl.multiple_of(n * chunk, chunk)
            piece = lax.dot_general(block, flat[pl.ds(at, chunk), :], NT, preferred_element_type=jnp.float32)
            score[:, pl.ds(at, chunk)] = piece * (depth ** -0.5)

        @pl.loop(0, local // 64)
        def _(g):
            tops = []
            for i in range(8):
                x = jnp.where(wide, score[pl.ds(pl.multiple_of(g * 64 + i * 8, 8), 8), :], -1e30)
                top = jnp.max(tree(lanes(x), jnp.maximum), axis=1, keepdims=True)
                tops.append(jnp.maximum(top, bin_value) - LIFT)
            for i, top in enumerate(tops):
                x = score[pl.ds(pl.multiple_of(g * 64 + i * 8, 8), 8), :]
                at = pl.multiple_of(s * local + g * 64 + i * 8, 8)
                kern[pl.ds(at, 8), :] = jnp.where(wide, jnp.exp(x - top), 0.0)
                full = jnp.broadcast_to(top, (8, LANES))
                peak[pl.ds(at, 8), :] = full
                kbin[pl.ds(at, 8), :] = jnp.exp(bin_value - full)
                index = at + lax.broadcasted_iota(jnp.int32, (8, LANES), 0)
                mass[pl.ds(at, 8), :] = jnp.where(index < na_i, norm, 0.0)

    for dz in range(teams):
        for d in range(1, size):
            fwd(0, dz, d).wait_recv()
    keeps.append(pltpu.make_async_copy(own, imgs.at[team], local_sem.at[0]))
    keeps[-1].start()

    def prepare_fwd(dz):
        for d in range(1, size):
            fwd(1, dz, d).wait_recv()
        for d in range(1, size):
            prepare((team + teams - dz) % teams, (member + size - d) % size)

    prepare(team, member)
    behind = 0
    for k in ranks:
        dz = near(k, -1)
        crit(1, dz).wait_recv()
        hand_over(1, dz)
        prepare_fwd(behind)
        prepare((team + teams - dz) % teams, member)
        behind = dz
    prepare_fwd(behind)
    for e in range(1, teams):
        pass_on(0, e)

    b8[...] = jnp.where(wide, 1.0, 0.0)
    bbin[...] = jnp.ones_like(bbin)
    groups = BLOCK // 8

    def row_part(g):
        ats = [pl.ds(pl.multiple_of(g * BLOCK + i * 8, 8), 8) for i in range(groups)]
        accs = [None] * groups
        for c in spans:
            span = slice(c * LANES, (c + 1) * LANES)
            weight = b8[:, span]
            for i, at in enumerate(ats):
                term = kern[at, span] * weight
                accs[i] = term if c == 0 else accs[i] + term
        for i, at in enumerate(ats):
            part[at, :] = accs[i]

    def row_close(g):
        edge = bbin[...]
        ats = [pl.ds(pl.multiple_of(g * BLOCK + i * 8, 8), 8) for i in range(groups)]
        totals = [jnp.broadcast_to(jnp.sum(part[at, :], axis=1, keepdims=True), (8, LANES)) + kbin[at, :] * edge for at in ats]
        for at, total in zip(ats, totals):
            left[at, :] = mass[at, :] / total

    def col_part(g, sums):
        sums = list(sums)
        for i in range(groups):
            at = pl.ds(pl.multiple_of(g * BLOCK + i * 8, 8), 8)
            a = left[at, :]
            for c in spans:
                sums[c] = sums[c] + kern[at, c * LANES : (c + 1) * LANES] * a
            sums[-1] = sums[-1] + kbin[at, :] * a
        return tuple(sums)

    def sweep(it, _):
        row_part(0)
        row_close(0)
        row_part(1)

        def step(g, sums):
            sums = col_part(g - 2, sums)
            row_close(g - 1)
            row_part(g)
            return sums

        zero = jnp.zeros((8, LANES), jnp.float32)
        sums = tuple(zero for _ in spans) + (zero,)
        sums = col_part(blocks - 2, lax.fori_loop(2, blocks, step, sums))
        row_close(blocks - 1)
        sums = col_part(blocks - 1, sums)
        all_b = jnp.sum(tree(lanes(b8[0:1, :]), jnp.add), axis=1, keepdims=True) + bbin[0:1, :1]
        row_bin = mu_bin / all_b
        abin[...] = row_bin
        for c in spans:
            span = slice(c * LANES, (c + 1) * LANES)
            fresh = norm / (jnp.sum(sums[c], axis=0, keepdims=True) + row_bin)
            fin_send[0, :, span] = fresh
            b8[:, span] = jnp.where(wide[:, span], fresh, 0.0)
        edge = jnp.sum(sums[-1], axis=0, keepdims=True) + row_bin
        bbin[...] = jnp.broadcast_to(nu_bin / edge, bbin.shape)
        for k, (dz, e) in enumerate(order):
            @pl.when(it == min(ITERS - 1, k * ITERS // len(order)))
            def _():
                bulk(dz, e).wait_recv()
                pass_on(dz, e)
        return 0

    lax.fori_loop(0, ITERS, sweep, 0)

    col_pot = jnp.log(fin_send[0, :, :cols])
    col_bin = jnp.log(bbin[0:1, :])
    row_bin = jnp.log(abin[...]) - bin_value
    eye = lax.broadcasted_iota(jnp.int32, (LANES, LANES), 0) == lax.broadcasted_iota(jnp.int32, (LANES, LANES), 1)
    for t in range(teams):
        fin_send[t, :, :cols] = col_pot
        fin_send[t, :, cols : cols + LANES] = col_bin
        fin_send[t, :, cols + LANES : cols + 2 * LANES] = row_bin
        for i in range(local // LANES):
            at = pl.ds(pl.multiple_of((t * size + member) * local + i * LANES, LANES), LANES)
            pot = jnp.log(jnp.maximum(left[at, :], 1e-37)) - peak[at, :]
            flat_pot = jnp.sum(jnp.where(eye, pot, 0.0), axis=0, keepdims=True)
            fin_send[t, :, cols + (2 + i) * LANES : cols + (3 + i) * LANES] = flat_pot
    sent = []
    for dz in range(1, teams):
        to = (team + dz) % teams
        sent.append(remote(fin_send.at[to], fin.at[team], fin_ssem.at[dz], fin_rsem.at[dz], to, member))
        sent[-1].start()
    fin[team] = fin_send[team]

    for kind in (0, 1):
        for dz in range(teams):
            if dz:
                crit(kind, dz).wait_send()
            for d in range(1, size):
                fwd(kind, dz, d).wait_send()
    for keep in keeps:
        keep.wait()
    for dz, e in order:
        bulk(dz, e).wait_send()
    for dz in range(teams):
        for e in range(1, teams):
            for d in range(1, size):
                side(dz, e, d).wait()
    for copy in sent:
        copy.wait()


def finish_kernel(size, counts, pairs, bin_score, rowdesc, image, fin, log_match, row_bins, col_bins):
    p = pl.program_id(0)
    me = lax.axis_index("row")
    local, depth = rowdesc.shape[1:]
    cols = log_match.shape[2]
    na_i, nb_i = counts[pairs[p, 0]], counts[pairs[p, 1]]
    line = jnp.ones((1, LANES), jnp.float32)
    log_norm = -jnp.log(line * (na_i + nb_i).astype(jnp.float32))[:, :1]
    bin_value = bin_score[0]
    col_pot = fin[0, :, :cols]
    col_bin = fin[0, :, cols : cols + 1]
    row_bin = fin[0, :, cols + LANES : cols + LANES + 1]
    flat_pot = fin[0, :, cols + 2 * LANES :]
    wide = lax.broadcasted_iota(jnp.int32, (1, cols), 1) < nb_i
    row_index = me * local + lax.broadcasted_iota(jnp.int32, (1, local), 1)
    row_bins[pl.ds(p, 1), :] = jnp.where(row_index < na_i, bin_value + flat_pot + col_bin - log_norm, 0.0)
    col_bins[pl.ds(p, 1), :] = jnp.where(wide, bin_value + row_bin + col_pot - log_norm, 0.0)
    eye = lax.broadcasted_iota(jnp.int32, (LANES, LANES), 0) == lax.broadcasted_iota(jnp.int32, (LANES, LANES), 1)
    tops = []
    for i in range(local // LANES):
        piece = flat_pot[:, i * LANES : (i + 1) * LANES]
        tops.append(jnp.sum(jnp.where(eye, piece, 0.0), axis=1, keepdims=True))
    row_pot = jnp.concatenate(tops, axis=0)
    tall = me * local + lax.broadcasted_iota(jnp.int32, (local, 1), 0) < na_i
    flat = image.reshape(cols, depth)
    chunk = 512 if cols % 512 == 0 else LANES
    block = rowdesc[0]
    for n in range(cols // chunk):
        at = slice(n * chunk, (n + 1) * chunk)
        scores = lax.dot_general(block, flat[at, :], NT, preferred_element_type=jnp.float32) * (depth ** -0.5)
        value = scores + row_pot + col_pot[:, at] - log_norm
        log_match[0, :, at] = jnp.where(tall & wide[:, at], value, 0.0)


def on_device(teams, size, descriptors, counts, pairs, bin_score):
    images, local, depth = descriptors.shape
    cols = local * teams * size
    width = cols + 2 * LANES + local
    vmem = pl.BlockSpec(memory_space=pltpu.VMEM)
    smem = pl.BlockSpec(memory_space=pltpu.SMEM)
    f32, bf16 = jnp.float32, jnp.bfloat16
    dma = pltpu.SemaphoreType.DMA
    imgs, fin = pl.pallas_call(
        functools.partial(sinkhorn_kernel, teams, size),
        out_shape=(
            jax.ShapeDtypeStruct((teams, teams, size, local, depth), bf16),
            jax.ShapeDtypeStruct((teams, 1, width), f32),
        ),
        in_specs=[smem, smem, smem, vmem],
        out_specs=(pl.BlockSpec(memory_space=pl.ANY), vmem),
        scratch_shapes=[
            pltpu.VMEM((teams, local, depth), bf16),
            pltpu.VMEM((teams, local, depth), bf16),
            pltpu.VMEM((teams, size, local, depth), bf16),
            pltpu.VMEM((teams, size, local, depth), bf16),
            pltpu.VMEM((local, cols), f32),
            pltpu.VMEM((cols, cols), f32),
            pltpu.VMEM((cols, LANES), f32),
            pltpu.VMEM((cols, LANES), f32),
            pltpu.VMEM((cols, LANES), f32),
            pltpu.VMEM((cols, LANES), f32),
            pltpu.VMEM((cols, LANES), f32),
            pltpu.VMEM((8, cols), f32),
            pltpu.VMEM((8, LANES), f32),
            pltpu.VMEM((1, LANES), f32),
            pltpu.VMEM((teams, 1, width), f32),
            dma((2, teams)),
            dma((2, teams)),
            dma((2, teams, size)),
            dma((2, teams, size)),
            dma((teams, teams)),
            dma((teams, teams)),
            dma((teams, teams, size)),
            dma((teams, teams, size)),
            dma((teams,)),
            dma((teams,)),
            dma((teams,)),
        ],
        compiler_params=pltpu.CompilerParams(
            collective_id=0, has_side_effects=True, vmem_limit_bytes=48 * 1024 * 1024
        ),
    )(counts, pairs, bin_score, descriptors)
    return pl.pallas_call(
        functools.partial(finish_kernel, size),
        out_shape=(
            jax.ShapeDtypeStruct((teams, local, cols), f32),
            jax.ShapeDtypeStruct((teams, local), f32),
            jax.ShapeDtypeStruct((teams, cols), f32),
        ),
        grid_spec=pltpu.PrefetchScalarGridSpec(
            num_scalar_prefetch=3,
            grid=(teams,),
            in_specs=[
                pl.BlockSpec((1, local, depth), lambda p, c, q, b: (q[p, 0], 0, 0)),
                pl.BlockSpec((1, teams, size, local, depth), lambda p, c, q, b: (p, 0, 0, 0, 0)),
                pl.BlockSpec((1, 1, width), lambda p, c, q, b: (p, 0, 0)),
            ],
            out_specs=(
                pl.BlockSpec((1, local, cols), lambda p, c, q, b: (p, 0, 0)),
                pl.BlockSpec((teams, local), lambda p, c, q, b: (0, 0)),
                pl.BlockSpec((teams, cols), lambda p, c, q, b: (0, 0)),
            ),
        ),
    )(counts, pairs, bin_score, descriptors, imgs, fin)


def solution(mesh):
    group = mesh.shape["row"]

    def body(descriptors, counts, pairs, bin_score):
        teams = pairs.shape[0]
        return on_device(teams, group // teams, descriptors, counts, pairs, bin_score)

    return jax.shard_map(
        body,
        mesh=mesh,
        in_specs=(P("pair", "row", None), P("pair"), P("pair", None), P()),
        out_specs=(P("pair", "row", None), P("pair", "row"), P("pair", None)),
        check_vma=False,
    )
```

```python
import functools

import jax
import jax.numpy as jnp
from jax import lax
from jax.experimental import pallas as pl
from jax.experimental.pallas import tpu as pltpu
from jax.sharding import PartitionSpec as P

ITERS = 10
LIFT = 40.0
LANES = 128
BLOCK = 128
MESH = pl.DeviceIdType.MESH
NT = (((1,), (1,)), ((), ()))


def sinkhorn_kernel(
    teams, size, counts, pairs, bin_score, source_desc, imgs, fin,
    desc, rowsel, colsel, rows, own, score, kern, peak, kbin, mass, left, part, b8, bbin, abin, fin_send,
    crit_send, crit_recv, fwd_send, fwd_recv, bulk_send, bulk_recv, side_send, side_recv, fin_ssem, fin_rsem, local_sem, load_sem,
):
    me = lax.axis_index("row")
    team, member = me // size, me % size
    local, depth = rows.shape[2:]
    height, cols = kern.shape
    blocks = height // BLOCK

    def device(t, m):
        return {"row": t * size + m}

    def remote(src, dst, ssem, rsem, t, m):
        return pltpu.make_async_remote_copy(
            src_ref=src, dst_ref=dst, send_sem=ssem, recv_sem=rsem, device_id=device(t, m), device_id_type=MESH
        )

    load = pltpu.make_async_copy(source_desc, desc, load_sem)
    load.start()
    barrier = pltpu.get_barrier_semaphore()
    for dz in range(1, teams):
        pl.semaphore_signal(barrier, inc=1, device_id=device((team + dz) % teams, member), device_id_type=MESH)
    for d in range(1, size):
        pl.semaphore_signal(barrier, inc=1, device_id=device(team, (member + d) % size), device_id_type=MESH)

    load.wait()
    for p in range(teams):
        colsel[p] = desc[pairs[p, 1]]
        rowsel[p] = desc[pairs[p, 0]]
    own[team, member] = colsel[team]
    rows[team, member] = rowsel[team]
    pl.semaphore_wait(barrier, teams + size - 2)

    def near(k, sign):
        pick = 0
        for t in range(teams):
            ranked = sorted((o for o in range(teams) if o != t), key=lambda o: (abs(o - t), o))
            pick = pick + jnp.where(team == t, sign * (ranked[k] - t) % teams, 0)
        return pick

    held = ((colsel, own), (rowsel, rows))
    ranks = range(teams - 1)

    def crit(kind, dz):
        to = (team + dz) % teams
        src, dst = held[kind]
        return remote(src.at[to], dst.at[team, member], crit_send.at[kind, dz], crit_recv.at[kind, dz], to, member)

    def fwd(kind, dz, d):
        slot = held[kind][1].at[(team + teams - dz) % teams, member]
        return remote(slot, slot, fwd_send.at[kind, dz, d], fwd_recv.at[kind, dz, d], team, (member + d) % size)

    def hand_over(kind, dz):
        for d in range(1, size):
            fwd(kind, dz, d).start()

    for kind in (0, 1):
        for k in reversed(ranks):
            crit(kind, near(k, 1)).start()
        hand_over(kind, 0)

    def bulk(dz, e):
        to = (team + dz) % teams
        image = (to + e) % teams
        return remote(colsel.at[image], imgs.at[image, team, member], bulk_send.at[dz, e], bulk_recv.at[dz, e], to, member)

    def side(dz, e, d):
        source, image = (team + teams - dz) % teams, (team + e) % teams
        slot = imgs.at[image, source, member]
        src = slot if dz else colsel.at[image]
        return remote(src, slot, side_send.at[dz, e, d], side_recv.at[dz, e, d], team, (member + d) % size)

    def pass_on(dz, e):
        for d in range(1, size):
            side(dz, e, d).start()

    order = [(dz, e) for e in range(1, teams) for dz in range(1, teams)]
    for dz, e in order:
        bulk(dz, e).start()
    keeps = []
    for e in range(1, teams):
        image = (team + e) % teams
        keeps.append(pltpu.make_async_copy(colsel.at[image], imgs.at[image, team, member], local_sem.at[e]))
        keeps[-1].start()
    for k in ranks:
        dz = near(k, -1)
        crit(0, dz).wait_recv()
        hand_over(0, dz)

    na_i, nb_i = counts[pairs[team, 0]], counts[pairs[team, 1]]
    line = jnp.ones((1, LANES), jnp.float32)
    na, nb = line * na_i.astype(jnp.float32), line * nb_i.astype(jnp.float32)
    norm = 1.0 / (na + nb)
    mu_bin, nu_bin = nb * norm, na * norm
    bin_value = bin_score[0]
    wide = lax.broadcasted_iota(jnp.int32, (8, cols), 1) < nb_i
    chunk = 512 if cols % 512 == 0 else LANES
    flat = own.reshape(cols, depth)
    spans = range(cols // LANES)

    def tree(terms, op):
        while len(terms) > 1:
            terms = [op(terms[i], terms[i + 1]) if i + 1 < len(terms) else terms[i] for i in range(0, len(terms), 2)]
        return terms[0]

    def lanes(x):
        return [x[:, i * LANES : (i + 1) * LANES] for i in spans]

    def prepare(source, m):
        s = source * size + m
        block = rows[source, m]

        @pl.loop(0, cols // chunk)
        def _(n):
            at = pl.multiple_of(n * chunk, chunk)
            piece = lax.dot_general(block, flat[pl.ds(at, chunk), :], NT, preferred_element_type=jnp.float32)
            score[:, pl.ds(at, chunk)] = piece * (depth ** -0.5)

        @pl.loop(0, local // 64)
        def _(g):
            tops = []
            for i in range(8):
                x = jnp.where(wide, score[pl.ds(pl.multiple_of(g * 64 + i * 8, 8), 8), :], -1e30)
                top = jnp.max(tree(lanes(x), jnp.maximum), axis=1, keepdims=True)
                tops.append(jnp.maximum(top, bin_value) - LIFT)
            for i, top in enumerate(tops):
                x = score[pl.ds(pl.multiple_of(g * 64 + i * 8, 8), 8), :]
                at = pl.multiple_of(s * local + g * 64 + i * 8, 8)
                kern[pl.ds(at, 8), :] = jnp.where(wide, jnp.exp(x - top), 0.0)
                full = jnp.broadcast_to(top, (8, LANES))
                peak[pl.ds(at, 8), :] = full
                kbin[pl.ds(at, 8), :] = jnp.exp(bin_value - full)
                index = at + lax.broadcasted_iota(jnp.int32, (8, LANES), 0)
                mass[pl.ds(at, 8), :] = jnp.where(index < na_i, norm, 0.0)

    for dz in range(teams):
        for d in range(1, size):
            fwd(0, dz, d).wait_recv()
    keeps.append(pltpu.make_async_copy(own, imgs.at[team], local_sem.at[0]))
    keeps[-1].start()

    def prepare_fwd(dz):
        for d in range(1, size):
            fwd(1, dz, d).wait_recv()
        for d in range(1, size):
            prepare((team + teams - dz) % teams, (member + size - d) % size)

    prepare(team, member)
    behind = 0
    for k in ranks:
        dz = near(k, -1)
        crit(1, dz).wait_recv()
        hand_over(1, dz)
        prepare_fwd(behind)
        prepare((team + teams - dz) % teams, member)
        behind = dz
    prepare_fwd(behind)
    for e in range(1, teams):
        pass_on(0, e)

    b8[...] = jnp.where(wide, 1.0, 0.0)
    bbin[...] = jnp.ones_like(bbin)
    groups = BLOCK // 8

    def row_part(g):
        ats = [pl.ds(pl.multiple_of(g * BLOCK + i * 8, 8), 8) for i in range(groups)]
        accs = [None] * groups
        for c in spans:
            span = slice(c * LANES, (c + 1) * LANES)
            weight = b8[:, span]
            for i, at in enumerate(ats):
                term = kern[at, span] * weight
                accs[i] = term if c == 0 else accs[i] + term
        for i, at in enumerate(ats):
            part[at, :] = accs[i]

    def row_close(g):
        edge = bbin[...]
        ats = [pl.ds(pl.multiple_of(g * BLOCK + i * 8, 8), 8) for i in range(groups)]
        totals = [jnp.broadcast_to(jnp.sum(part[at, :], axis=1, keepdims=True), (8, LANES)) + kbin[at, :] * edge for at in ats]
        for at, total in zip(ats, totals):
            left[at, :] = mass[at, :] / total

    def col_part(g, sums):
        sums = list(sums)
        for i in range(groups):
            at = pl.ds(pl.multiple_of(g * BLOCK + i * 8, 8), 8)
            a = left[at, :]
            for c in spans:
                sums[c] = sums[c] + kern[at, c * LANES : (c + 1) * LANES] * a
            sums[-1] = sums[-1] + kbin[at, :] * a
        return tuple(sums)

    def sweep(it, _):
        row_part(0)
        row_close(0)
        row_part(1)

        def step(g, sums):
            sums = col_part(g - 2, sums)
            row_close(g - 1)
            row_part(g)
            return sums

        zero = jnp.zeros((8, LANES), jnp.float32)
        sums = tuple(zero for _ in spans) + (zero,)
        sums = col_part(blocks - 2, lax.fori_loop(2, blocks, step, sums))
        row_close(blocks - 1)
        sums = col_part(blocks - 1, sums)
        all_b = jnp.sum(tree(lanes(b8[0:1, :]), jnp.add), axis=1, keepdims=True) + bbin[0:1, :1]
        row_bin = mu_bin / all_b
        abin[...] = row_bin
        for c in spans:
            span = slice(c * LANES, (c + 1) * LANES)
            fresh = norm / (jnp.sum(sums[c], axis=0, keepdims=True) + row_bin)
            fin_send[0, :, span] = fresh
            b8[:, span] = jnp.where(wide[:, span], fresh, 0.0)
        edge = jnp.sum(sums[-1], axis=0, keepdims=True) + row_bin
        bbin[...] = jnp.broadcast_to(nu_bin / edge, bbin.shape)
        for k, (dz, e) in enumerate(order):
            @pl.when(it == min(ITERS - 1, k * ITERS // len(order)))
            def _():
                bulk(dz, e).wait_recv()
                pass_on(dz, e)
        return 0

    lax.fori_loop(0, ITERS, sweep, 0)

    col_pot = jnp.log(fin_send[0, :, :cols])
    col_bin = jnp.log(bbin[0:1, :])
    row_bin = jnp.log(abin[...]) - bin_value
    eye = lax.broadcasted_iota(jnp.int32, (LANES, LANES), 0) == lax.broadcasted_iota(jnp.int32, (LANES, LANES), 1)
    for t in range(teams):
        fin_send[t, :, :cols] = col_pot
        fin_send[t, :, cols : cols + LANES] = col_bin
        fin_send[t, :, cols + LANES : cols + 2 * LANES] = row_bin
        for i in range(local // LANES):
            at = pl.ds(pl.multiple_of((t * size + member) * local + i * LANES, LANES), LANES)
            pot = jnp.log(jnp.maximum(left[at, :], 1e-37)) - peak[at, :]
            flat_pot = jnp.sum(jnp.where(eye, pot, 0.0), axis=0, keepdims=True)
            fin_send[t, :, cols + (2 + i) * LANES : cols + (3 + i) * LANES] = flat_pot
    sent = []
    for dz in range(1, teams):
        to = (team + dz) % teams
        sent.append(remote(fin_send.at[to], fin.at[team], fin_ssem.at[dz], fin_rsem.at[dz], to, member))
        sent[-1].start()
    fin[team] = fin_send[team]

    for kind in (0, 1):
        for dz in range(teams):
            if dz:
                crit(kind, dz).wait_send()
            for d in range(1, size):
                fwd(kind, dz, d).wait_send()
    for keep in keeps:
        keep.wait()
    for dz, e in order:
        bulk(dz, e).wait_send()
    for dz in range(teams):
        for e in range(1, teams):
            for d in range(1, size):
                side(dz, e, d).wait()
    for copy in sent:
        copy.wait()


def finish_kernel(size, counts, pairs, bin_score, rowdesc, image, fin, log_match, row_bins, col_bins):
    p = pl.program_id(0)
    me = lax.axis_index("row")
    local, depth = rowdesc.shape[1:]
    cols = log_match.shape[2]
    na_i, nb_i = counts[pairs[p, 0]], counts[pairs[p, 1]]
    line = jnp.ones((1, LANES), jnp.float32)
    log_norm = -jnp.log(line * (na_i + nb_i).astype(jnp.float32))[:, :1]
    bin_value = bin_score[0]
    col_pot = fin[0, :, :cols]
    col_bin = fin[0, :, cols : cols + 1]
    row_bin = fin[0, :, cols + LANES : cols + LANES + 1]
    flat_pot = fin[0, :, cols + 2 * LANES :]
    wide = lax.broadcasted_iota(jnp.int32, (1, cols), 1) < nb_i
    row_index = me * local + lax.broadcasted_iota(jnp.int32, (1, local), 1)
    row_bins[pl.ds(p, 1), :] = jnp.where(row_index < na_i, bin_value + flat_pot + col_bin - log_norm, 0.0)
    col_bins[pl.ds(p, 1), :] = jnp.where(wide, bin_value + row_bin + col_pot - log_norm, 0.0)
    eye = lax.broadcasted_iota(jnp.int32, (LANES, LANES), 0) == lax.broadcasted_iota(jnp.int32, (LANES, LANES), 1)
    tops = []
    for i in range(local // LANES):
        piece = flat_pot[:, i * LANES : (i + 1) * LANES]
        tops.append(jnp.sum(jnp.where(eye, piece, 0.0), axis=1, keepdims=True))
    row_pot = jnp.concatenate(tops, axis=0)
    tall = me * local + lax.broadcasted_iota(jnp.int32, (local, 1), 0) < na_i
    flat = image.reshape(cols, depth)
    chunk = 512 if cols % 512 == 0 else LANES
    block = rowdesc[0]
    for n in range(cols // chunk):
        at = slice(n * chunk, (n + 1) * chunk)
        scores = lax.dot_general(block, flat[at, :], NT, preferred_element_type=jnp.float32) * (depth ** -0.5)
        value = scores + row_pot + col_pot[:, at] - log_norm
        log_match[0, :, at] = jnp.where(tall & wide[:, at], value, 0.0)


def on_device(teams, size, descriptors, counts, pairs, bin_score):
    images, local, depth = descriptors.shape
    cols = local * teams * size
    width = cols + 2 * LANES + local
    vmem = pl.BlockSpec(memory_space=pltpu.VMEM)
    smem = pl.BlockSpec(memory_space=pltpu.SMEM)
    f32, bf16 = jnp.float32, jnp.bfloat16
    dma = pltpu.SemaphoreType.DMA
    imgs, fin = pl.pallas_call(
        functools.partial(sinkhorn_kernel, teams, size),
        out_shape=(
            jax.ShapeDtypeStruct((teams, teams, size, local, depth), bf16),
            jax.ShapeDtypeStruct((teams, 1, width), f32),
        ),
        in_specs=[smem, smem, smem, pl.BlockSpec(memory_space=pl.ANY)],
        out_specs=(pl.BlockSpec(memory_space=pl.ANY), vmem),
        scratch_shapes=[
            pltpu.VMEM((images, local, depth), bf16),
            pltpu.VMEM((teams, local, depth), bf16),
            pltpu.VMEM((teams, local, depth), bf16),
            pltpu.VMEM((teams, size, local, depth), bf16),
            pltpu.VMEM((teams, size, local, depth), bf16),
            pltpu.VMEM((local, cols), f32),
            pltpu.VMEM((cols, cols), f32),
            pltpu.VMEM((cols, LANES), f32),
            pltpu.VMEM((cols, LANES), f32),
            pltpu.VMEM((cols, LANES), f32),
            pltpu.VMEM((cols, LANES), f32),
            pltpu.VMEM((cols, LANES), f32),
            pltpu.VMEM((8, cols), f32),
            pltpu.VMEM((8, LANES), f32),
            pltpu.VMEM((1, LANES), f32),
            pltpu.VMEM((teams, 1, width), f32),
            dma((2, teams)),
            dma((2, teams)),
            dma((2, teams, size)),
            dma((2, teams, size)),
            dma((teams, teams)),
            dma((teams, teams)),
            dma((teams, teams, size)),
            dma((teams, teams, size)),
            dma((teams,)),
            dma((teams,)),
            dma((teams,)),
            dma,
        ],
        compiler_params=pltpu.CompilerParams(
            collective_id=0, has_side_effects=True, vmem_limit_bytes=60 * 1024 * 1024
        ),
    )(counts, pairs, bin_score, descriptors)
    return pl.pallas_call(
        functools.partial(finish_kernel, size),
        out_shape=(
            jax.ShapeDtypeStruct((teams, local, cols), f32),
            jax.ShapeDtypeStruct((teams, local), f32),
            jax.ShapeDtypeStruct((teams, cols), f32),
        ),
        grid_spec=pltpu.PrefetchScalarGridSpec(
            num_scalar_prefetch=3,
            grid=(teams,),
            in_specs=[
                pl.BlockSpec((1, local, depth), lambda p, c, q, b: (q[p, 0], 0, 0)),
                pl.BlockSpec((1, teams, size, local, depth), lambda p, c, q, b: (p, 0, 0, 0, 0)),
                pl.BlockSpec((1, 1, width), lambda p, c, q, b: (p, 0, 0)),
            ],
            out_specs=(
                pl.BlockSpec((1, local, cols), lambda p, c, q, b: (p, 0, 0)),
                pl.BlockSpec((teams, local), lambda p, c, q, b: (0, 0)),
                pl.BlockSpec((teams, cols), lambda p, c, q, b: (0, 0)),
            ),
        ),
    )(counts, pairs, bin_score, descriptors, imgs, fin)


def solution(mesh):
    group = mesh.shape["row"]

    def body(descriptors, counts, pairs, bin_score):
        teams = pairs.shape[0]
        return on_device(teams, group // teams, descriptors, counts, pairs, bin_score)

    return jax.shard_map(
        body,
        mesh=mesh,
        in_specs=(P("pair", "row", None), P("pair"), P("pair", None), P()),
        out_specs=(P("pair", "row", None), P("pair", "row"), P("pair", None)),
        check_vma=False,
    )
```
